256 devices in a mesh: seq: 32 (over x, z), batch: 8 (over y, core).
Axes of the slice: x: 4, y: 4, z: 8, core: 2. Of those that a mesh axis runs over, the one named last changes fastest.
Arguments:
- hidden: bfloat16 [16, 8192, 4096], P('batch', None, 'seq')
- gain: float32 [4096], P('seq'), may hold values from 0.5 to 1.5
- value_weight: float32 [4096], P('seq'), may hold values from -0.09375 to 0.09375
- rewards: float32 [16, 8192], P('batch', 'seq'), may hold values from -1.5 to 1.5
- reward_mask: int32 [16, 8192], P('batch', 'seq'), may hold values 0 or 1
- lengths: int32 [16], P('batch'), may hold values from 2048 to 8192
- horizon: float32 [16], P('batch'), may hold values from 24 to 65536
Outputs:
- advantages: float32 [16, 8192], P(None, ('seq', 'batch'))
- returns: float32 [16, 8192], P(None, ('seq', 'batch'))
The draws below stay inside these ranges and needn't reach their ends.
All inputs are finite; a program needn't handle non-finite values. No bound on the sum of `reward_mask` on one device may be relied on, other than what follows from the above.
Results may differ from the reference program's by a relative error of at most 0.0003.
Values may be sent and summed in bfloat16 or wider, within the bound.
A program may use at most 64 MiB of HBM per device.

```python
import jax
import jax.numpy as jnp
from jax import lax

D = 4096
B = 16
S = 8192


def draw_hidden(key, part):
    first_key = jax.random.fold_in(key, 11)
    second_key = jax.random.fold_in(key, 12)
    base = jax.random.normal(first_key, (B, S, D), jnp.float32)
    scales = jnp.exp(jax.random.uniform(second_key, (B, S, D // 16, 1), jnp.float32, -1.2, 1.2))
    return (base.reshape(B, S, D // 16, 16) * scales).reshape(B, S, D).astype(jnp.bfloat16)


def draw_horizon(key, part):
    inner = jax.random.fold_in(key, 21)
    lower = jnp.log(24.0)
    upper = jnp.log(4.0 * S)
    return jnp.exp(jax.random.uniform(inner, (B,), jnp.float32, lower, upper)).astype(jnp.float32)


def place_ends(drawn, rng, least, high):
    dims = drawn.shape
    index_at = [jax.random.randint(jax.random.fold_in(rng, axis), (), 0, dims[axis]) for axis in range(len(dims))]
    drawn = drawn.at[tuple(index_at)].set(least)
    longest = dims.index(max(dims))
    index_at[longest] = (index_at[longest] + 1) % dims[longest]
    return drawn.at[tuple(index_at)].set(high)


def level_of(key, dims, shards, low, high):
    factor_of = 1.0
    for axis_at, parts in shards:
        steps = jax.random.uniform(jax.random.fold_in(jax.random.fold_in(key, 6), axis_at), (parts,), jnp.float32, low / len(shards), high / len(shards))
        factor_of = factor_of * jnp.repeat(jnp.exp(steps), dims[axis_at] // parts).reshape((-1,) + (1,) * (len(dims) - 1 - axis_at))
    return factor_of


def normal_values(own_key, dims, scale, limit, split=(), held_as=jnp.bfloat16):
    result = scale * jax.random.normal(own_key, dims, jnp.float32)
    if split:
        result = result * level_of(own_key, dims, split, -0.22, 0.18)
    return jnp.clip(result, -limit, limit).astype(held_as)


def setup_inputs(seed: int = 0) -> dict:
    splits = jax.random.split(jax.random.key(seed), 8)
    return {
        "hidden": draw_hidden(jax.random.fold_in(splits[7], 71), 0),
        "gain": jnp.clip(1.0 + 0.1 * jax.random.normal(splits[1], (D,), jnp.float32), 0.5, 1.5),
        "value_weight": normal_values(splits[2], (D,), D ** -0.5, 0.09375, ((0, 32),), jnp.float32),
        "rewards": normal_values(splits[3], (B, S), 0.1, 1.5, ((0, 8), (1, 32)), jnp.float32),
        "reward_mask": place_ends((jax.random.randint(splits[4], (B, S), 0, 4) < 1).astype(jnp.int32), jax.random.fold_in(splits[4], 1), 0, 1),
        "lengths": place_ends(jax.random.randint(splits[5], (B,), S // 4, S + 1), jax.random.fold_in(splits[5], 1), S // 4, S).astype(jnp.int32),
        "horizon": draw_horizon(jax.random.fold_in(splits[7], 71), 0),
    }


EPS = 1e-05

def reference(hidden, gain, value_weight, rewards, reward_mask, lengths, horizon):
    head_vec = gain * value_weight

    def head(rows):
        wide_rows = rows.astype(jnp.float32)
        return lax.optimization_barrier(jnp.sum(wide_rows * head_vec, -1)) * lax.rsqrt(lax.optimization_barrier(jnp.mean(wide_rows * wide_rows, -1)) + EPS)
    values = lax.map(head, hidden)
    length_all = hidden.shape[1]
    positions = jnp.arange(length_all, dtype=jnp.int32)
    valid = (positions[None, :] < lengths[:, None]).astype(jnp.float32)
    next_valid = (positions[None, :] + 1 < lengths[:, None]).astype(jnp.float32)
    next_values = jnp.concatenate([values[:, 1:], jnp.zeros((values.shape[0], 1), jnp.float32)], 1)
    delta = (rewards * reward_mask.astype(jnp.float32) + next_valid * next_values - values) * valid
    decay = jnp.exp(-1.0 / horizon)

    def step(carry, inputs):
        d_now, v_next = inputs
        fresh = d_now + decay * v_next * carry
        return (fresh, fresh)
    _, gae_t = lax.scan(step, jnp.zeros(values.shape[0], jnp.float32), (delta.T, next_valid.T), reverse=True)
    gae = gae_t.T
    returns = (gae + values) * valid
    count = jnp.sum(valid)
    first = jnp.sum(gae)
    second = jnp.sum(gae * gae)
    mean = first / count
    var = jnp.maximum(second / count - mean * mean, 1.0)
    advantages = (gae - mean) * valid * lax.rsqrt(var)
    return (advantages, returns)
```

```python
import jax
import jax.numpy as jnp
from jax import lax
from jax.experimental import pallas as pl
from jax.experimental.pallas import tpu as pltpu
from jax.sharding import PartitionSpec as P

D = 4096
EPS = 1e-05
NX, NZ = 4, 8
NS = NX * NZ
NB = 8
BLOCK = 256
CHUNKS = 8
PER_CHUNK = NS // CHUNKS
MESH = pl.DeviceIdType.MESH
F32 = jnp.float32
BF16 = jnp.bfloat16


def ring(d, n):
    return min(d, n - d)


OFFSETS = sorted(
    ((dx, dz) for dx in range(NX) for dz in range(NZ) if dx or dz),
    key=lambda o: (-(ring(o[0], NX) + ring(o[1], NZ)), o),
)


def iota(shape, dim):
    return lax.broadcasted_iota(jnp.int32, shape, dim)


def kernel(
    hidden, gain, weight, rewards, mask, lengths, horizon, adv_ref, ret_ref,
    hv, gv, wv, rv, mv, lens, hors, send1, recv1, send2, recv2, send3, recv3,
    hsem, gsem, isem, ssem, rsem,
):
    me, mb = lax.axis_index("seq"), lax.axis_index("batch")
    mx, mz = me // NZ, me % NZ
    span = CHUNKS and hv.shape[1] // CHUNKS

    def chunk_copy(c):
        at = pl.ds(pl.multiple_of(c * span, span), span)
        return pltpu.make_async_copy(hidden.at[:, at], hv.at[:, at], hsem.at[c])

    def peer(dx, dz):
        return lax.rem(mx + dx, NX) * NZ + lax.rem(mz + dz, NZ)

    def batch_peer(k):
        return lax.rem(mb + k, NB)

    weights = [
        pltpu.make_async_copy(gain, gv, gsem.at[0]),
        pltpu.make_async_copy(weight, wv, gsem.at[1]),
    ]
    for copy in weights:
        copy.start()
    for c in range(CHUNKS):
        chunk_copy(c).start()
    smalls = [
        pltpu.make_async_copy(src, dst, isem.at[k])
        for k, (src, dst) in enumerate(
            ((rewards, rv), (mask, mv), (lengths, lens), (horizon, hors))
        )
    ]
    for copy in smalls:
        copy.start()

    barrier = pltpu.get_barrier_semaphore()
    for dx, dz in OFFSETS:
        pl.semaphore_signal(barrier, inc=1, device_id={"seq": peer(dx, dz)}, device_id_type=MESH)
    for k in range(1, NB):
        pl.semaphore_signal(barrier, inc=1, device_id={"batch": batch_peer(k)}, device_id_type=MESH)

    for copy in weights:
        copy.wait()
    head = gv[...].reshape(1, 128) * wv[...].reshape(1, 128)
    high = head.astype(BF16).astype(F32)
    middle = (head - high).astype(BF16).astype(F32)
    low = head - high - middle
    row16 = iota((16, 128), 0)
    left = jnp.where(row16 == 0, high, jnp.where(row16 == 1, middle, jnp.where(row16 == 2, low, 0.0)))
    left = left.astype(BF16)
    ones = jnp.ones((16, 256), BF16)
    row = iota((8, 128), 0)
    lane = iota((8, 128), 1)
    across = (((1,), (1,)), ((), ()))

    def sums_of_chunk(c, _):
        chunk_copy(c).wait()
        for i in range(PER_CHUNK):
            block = c * PER_CHUNK + i
            tile = jnp.zeros((8, 128), F32)
            for r in range(2):
                h = hv[r, pl.ds(pl.multiple_of(block * BLOCK, BLOCK), BLOCK), :]
                wide = h.astype(F32)
                square = wide * wide
                square_high = square.astype(BF16)
                square_low = (square - square_high.astype(F32)).astype(BF16)
                parts = lax.dot_general(left, h, across, preferred_element_type=F32)
                projected = jnp.sum(parts[0:8], axis=0, keepdims=True)
                both = jnp.concatenate([square_high, square_low], axis=1)
                squares = lax.dot_general(ones, both, across, preferred_element_type=F32)[0:8]
                for half in range(2):
                    at = slice(half * 128, half * 128 + 128)
                    k = r * 2 + half
                    tile = jnp.where(row == k, squares[:, at], tile)
                    tile = jnp.where(row == k + 4, projected[:, at], tile)
            send1[block] = tile
        return 0

    lax.fori_loop(0, CHUNKS, sums_of_chunk, 0)

    pl.semaphore_wait(barrier, NS - 1 + NB - 1)

    def first_copy(dx, dz):
        return pltpu.make_async_remote_copy(
            src_ref=send1.at[peer(dx, dz)],
            dst_ref=recv1.at[dx * NZ + dz - 1],
            send_sem=ssem.at[0],
            recv_sem=rsem.at[0],
            device_id={"seq": peer(dx, dz)},
            device_id_type=MESH,
        )

    for dx, dz in OFFSETS:
        first_copy(dx, dz).start()

    for copy in smalls:
        copy.wait()
    resp = (row >> 1) & 1
    half = row & 1
    length = jnp.where(resp == 0, lens[0], lens[1])
    position = me * BLOCK + half * 128 + lane
    valid = (position < length).astype(F32)
    next_valid = (position + 1 < length).astype(F32)
    rate = -1.0 / jnp.where(resp == 0, hors[0], hors[1])
    inside = half * 128 + lane
    steps = [
        jnp.where(lane < 128 - (1 << i), jnp.exp(rate * float(1 << i)), 0.0) for i in range(7)
    ]
    over_half = jnp.where(half == 0, jnp.exp(rate * (128 - lane).astype(F32)), 0.0)
    tail = jnp.exp(rate * (255 - inside).astype(F32))
    reward4 = jnp.concatenate(
        [rv[r : r + 1, h * 128 : h * 128 + 128] * mv[r : r + 1, h * 128 : h * 128 + 128].astype(F32)
         for _ in range(2) for r in range(2) for h in range(2)], axis=0)
    reward4 = reward4 * valid

    def per_response(x):
        both = x + pltpu.roll(x, 7, 0)
        return jnp.sum(both, axis=1, keepdims=True)

    def by_lane(column):
        wide = jnp.broadcast_to(column, (8, 128))
        return jnp.where(lane[0:1] < 64, wide[0:1], wide[2:3])

    tails = by_lane(per_response(tail))
    tails2 = by_lane(per_response(tail * tail))
    lane32 = iota((NS, 128), 1)
    j = iota((NS, 128), 0)
    rate32 = -1.0 / jnp.where(lane32 < 64, hors[0], hors[1])
    length32 = jnp.where(lane32 < 64, lens[0], lens[1])
    more = ((j + 1) * BLOCK < length32).astype(F32)
    block_steps = [
        jnp.where(j < NS - (1 << i), jnp.exp(rate32 * float(BLOCK << i)), 0.0) for i in range(5)
    ]
    to_start = jnp.exp(rate32 * float(BLOCK - 1)) * more
    once = jnp.where(j < NS - 1, jnp.exp(rate32), 0.0)

    def arrived(buffer, count, sem):
        whole = buffer.at[pl.ds(0, count)]
        pltpu.make_async_remote_copy(
            src_ref=whole, dst_ref=whole, send_sem=ssem.at[0], recv_sem=sem,
            device_id={"seq": peer(0, 1)}, device_id_type=MESH,
        ).wait_recv()

    arrived(recv1, NS - 1, rsem.at[0])
    total = send1[me] + jnp.sum(recv1[...], axis=0)
    other = pltpu.roll(total, 4, 0)
    squares = jnp.where(row < 4, total, other)
    projected = jnp.where(row < 4, other, total)
    values = projected * lax.rsqrt(squares * (1.0 / D) + EPS)
    following = pltpu.roll(values, 127, 1)
    following = jnp.where(
        lane == 127, jnp.where(half == 0, pltpu.roll(following, 7, 0), 0.0), following
    )
    x = reward4 + (next_valid * following - values) * valid
    for i in range(7):
        x = x + steps[i] * pltpu.roll(x, 128 - (1 << i), 1)
    x = x + over_half * jnp.broadcast_to(pltpu.roll(x, 7, 0)[:, 0:1], (8, 128))

    columns = (
        x[:, 0:1], values[:, 0:1], per_response(x), per_response(x * x), per_response(x * tail)
    )
    packed = jnp.zeros((8, 128), F32)
    for k, column in enumerate(columns):
        packed = jnp.where((lane & 63) == k, column, packed)
    message = jnp.where(lane[0:1] < 64, packed[0:1], packed[2:3])
    send2[...] = message
    recv2[me] = message

    def second_copy(dx, dz):
        return pltpu.make_async_remote_copy(
            src_ref=send2,
            dst_ref=recv2.at[me],
            send_sem=ssem.at[1],
            recv_sem=rsem.at[1],
            device_id={"seq": peer(dx, dz)},
            device_id_type=MESH,
        )

    for dx, dz in OFFSETS:
        second_copy(dx, dz).start()
    arrived(recv2, NS - 1, rsem.at[1])

    start = recv2[...].reshape(NS, 128)
    first_value, sum1, sum2, cross = (pltpu.roll(start, 128 - k, 1) for k in range(1, 5))
    next_first = pltpu.roll(first_value, NS - 1, 0)
    g = start + to_start * next_first
    for i in range(5):
        g = g + block_steps[i] * pltpu.roll(g, NS - (1 << i), 0)
    carry = once * pltpu.roll(g, NS - 1, 0) + more * next_first
    first = jnp.sum(sum1 + carry * tails, axis=0, keepdims=True)
    second = jnp.sum(sum2 + carry * (2.0 * cross + carry * tails2), axis=0, keepdims=True)
    mine = jnp.sum(jnp.where(j == me, carry, 0.0), axis=0, keepdims=True)
    gae = x + tail * jnp.where(resp == 0, mine[:, 0:1], mine[:, 64:65])
    returns = (gae + values) * valid
    tokens = (lens[0] + lens[1]).astype(F32)
    first = jnp.where(lane[0:1] == 1, tokens, first)
    for h in range(2):
        rows = (
            gae[h : h + 1], gae[2 + h : 3 + h], returns[h : h + 1], returns[2 + h : 3 + h],
            valid[h : h + 1], valid[2 + h : 3 + h], first, second,
        )
        send3[h] = jnp.concatenate(rows, axis=0)
    recv3[mb] = send3[mb // 4]

    def third_copy(k):
        return pltpu.make_async_remote_copy(
            src_ref=send3.at[batch_peer(k) // 4],
            dst_ref=recv3.at[mb],
            send_sem=ssem.at[2],
            recv_sem=rsem.at[2],
            device_id={"batch": batch_peer(k)},
            device_id_type=MESH,
        )

    for k in range(1, NB):
        third_copy(k).start()
    arrived(recv3, NB - 1, rsem.at[2])
    got = recv3[...]
    sums = jnp.sum(got, axis=0)
    count = sums[6:7, 1:2]
    mean = (sums[6:7, 0:1] + sums[6:7, 64:65]) / count
    var = jnp.maximum((sums[7:8, 0:1] + sums[7:8, 64:65]) / count - mean * mean, 1.0)
    scale = lax.rsqrt(var)
    rows = lambda k: got[:, k : k + 2, :].reshape(2 * NB, 128)
    advantages = (rows(0) - mean) * rows(4) * scale
    back = lax.rem(128 - lax.rem(mb, 4) * 32, 128)
    adv_ref[...] = pltpu.roll(advantages, back, 1)[:, 0:32]
    ret_ref[...] = pltpu.roll(rows(2), back, 1)[:, 0:32]

    def sent(buffer, count, sem):
        whole = buffer.at[pl.ds(0, count)]
        pltpu.make_async_remote_copy(
            src_ref=whole, dst_ref=whole, send_sem=sem, recv_sem=rsem.at[0],
            device_id={"seq": peer(0, 1)}, device_id_type=MESH,
        ).wait_send()

    sent(recv1, NS - 1, ssem.at[0])
    sent(recv2, NS - 1, ssem.at[1])
    sent(recv3, NB - 1, ssem.at[2])


def per_device(hidden, gain, weight, rewards, mask, lengths, horizon):
    responses, tokens, width = hidden.shape
    out = jax.ShapeDtypeStruct((2 * NB, 32), F32)
    return pl.pallas_call(
        kernel,
        name="critic_gae",
        out_shape=(out, out),
        in_specs=[pl.BlockSpec(memory_space=pltpu.HBM)] * 7,
        out_specs=(pl.BlockSpec(memory_space=pltpu.VMEM),) * 2,
        scratch_shapes=[
            pltpu.VMEM(hidden.shape, BF16),
            pltpu.VMEM(gain.shape, F32),
            pltpu.VMEM(weight.shape, F32),
            pltpu.VMEM(rewards.shape, F32),
            pltpu.VMEM(mask.shape, jnp.int32),
            pltpu.SMEM(lengths.shape, jnp.int32),
            pltpu.SMEM(horizon.shape, F32),
            pltpu.VMEM((NS, 8, 128), F32),
            pltpu.VMEM((NS - 1, 8, 128), F32),
            pltpu.VMEM((1, 128), F32),
            pltpu.VMEM((NS, 1, 128), F32),
            pltpu.VMEM((2, 8, 128), F32),
            pltpu.VMEM((NB, 8, 128), F32),
            pltpu.SemaphoreType.DMA((CHUNKS,)),
            pltpu.SemaphoreType.DMA((2,)),
            pltpu.SemaphoreType.DMA((4,)),
            pltpu.SemaphoreType.DMA((3,)),
            pltpu.SemaphoreType.DMA((3,)),
        ],
        compiler_params=pltpu.CompilerParams(collective_id=0, has_side_effects=True),
    )(hidden, gain, weight, rewards, mask, lengths, horizon)


def solution(mesh):
    return jax.shard_map(
        per_device,
        mesh=mesh,
        in_specs=(
            P("batch", None, "seq"), P("seq"), P("seq"), P("batch", "seq"), P("batch", "seq"),
            P("batch"), P("batch"),
        ),
        out_specs=(P(None, ("seq", "batch")), P(None, ("seq", "batch"))),
        check_vma=False,
    )
```
